128 devices in a mesh: pair: 16 (over x, z_lo, core), ga: 8 (over z_hi, y).
Axes of the slice: x: 4, y: 4, z: 4 (z_hi: 2, z_lo: 2; z = z_hi * 2 + z_lo), core: 2. Of those that a mesh axis runs over, the one named last changes fastest.
Arguments:
- densities: bfloat16 [24576, 4096], P('pair', 'ga'), may hold values from -6 to 6
- val_band: int32 [24576], P('pair'), may hold values from 0 to 127
- cond_band: int32 [24576], P('pair'), may hold values from 0 to 255
- val_energy: float32 [128], replicated, may hold values from -12 to -1
- cond_energy: float32 [256], replicated, may hold values from 1 to 12
Outputs:
- chi: float32 [4096, 4096], P('ga', 'pair')
The draws below stay inside these ranges and needn't reach their ends.
All inputs are finite; a program needn't handle non-finite values.
Results may differ from the reference program's by a relative error of at most 0.0012.
Values may be sent and summed in bfloat16 or wider, within the bound.
No kernel may reach another device: no remote copies, remote signals or barrier semaphores. Data moves between devices by JAX's collectives and lax.ppermute only.
A program may use at most 128 MiB of HBM per device.

```python
import math
import jax
import jax.numpy as jnp
from jax import lax

NG = 4096
NV = 128
NC = 256
P_DEV = 1536
PAIRS = 24576
N_PAIR = 16


def place_ends(array, stream_key, least, top_value):
    shape = array.shape
    index_at = [jax.random.randint(jax.random.fold_in(stream_key, axis), (), 0, shape[axis]) for axis in range(len(shape))]
    array = array.at[tuple(index_at)].set(least)
    longest = shape.index(max(shape))
    index_at[longest] = (index_at[longest] + 1) % shape[longest]
    return array.at[tuple(index_at)].set(top_value)


def steps_of(stream_key, shape, cuts, least, high):
    gain, own = 1.0, jax.random.fold_in(stream_key, 6)
    for axis_at, shards_of in cuts:
        heights = jnp.exp(jax.random.uniform(jax.random.fold_in(own, axis_at), (shards_of,), jnp.float32, least / len(cuts), high / len(cuts)))
        gain = gain * jnp.repeat(heights, shape[axis_at] // shards_of).reshape([-1 if axis == axis_at else 1 for axis in range(len(shape))])
    return gain


def gaussian(rng, shape, scale, most, shards=(), held_as=jnp.bfloat16):
    level = steps_of(rng, shape, shards, -0.22, 0.18) if shards else 1.0
    entries = jax.random.normal(rng, shape, jnp.float32) * scale * level
    return jnp.minimum(jnp.maximum(entries, -most), most).astype(held_as)


def setup_inputs(seed: int = 0) -> dict:
    arg_keys = jax.random.split(jax.random.key(seed), 6)
    return {
        "densities": gaussian(arg_keys[0], (PAIRS, NG), 1.0, 6.0, ((0, 16), (1, 8))),
        "val_band": place_ends(jax.random.randint(arg_keys[1], (PAIRS,), 0, NV), jax.random.fold_in(arg_keys[1], 1), 0, NV - 1).astype(jnp.int32),
        "cond_band": place_ends(jax.random.randint(arg_keys[2], (PAIRS,), 0, NC), jax.random.fold_in(arg_keys[2], 1), 0, NC - 1).astype(jnp.int32),
        "val_energy": jnp.clip(jax.random.uniform(arg_keys[3], (NV,), jnp.float32, -12.0, -1.0), -12.0, -1.0),
        "cond_energy": jnp.clip(jax.random.uniform(arg_keys[4], (NC,), jnp.float32, 1.0, 12.0), 1.0, 12.0),
    }


def reference(densities, val_band, cond_band, val_energy, cond_energy):
    gap = val_energy[val_band] - cond_energy[cond_band]
    weight = 4.0 / (gap * math.sqrt(PAIRS))
    scaled = (weight[:, None] * densities.astype(jnp.float32)).astype(jnp.bfloat16)
    left_groups = scaled.reshape(N_PAIR, P_DEV, NG)
    right_groups = densities.reshape(N_PAIR, P_DEV, NG)

    def add_group(total, pieces):
        left, right = pieces
        partial_value = lax.dot_general(left, right, (((0,), (0,)), ((), ())), preferred_element_type=jnp.float32)
        return (total + partial_value, None)
    total, unused = lax.scan(add_group, jnp.zeros((NG, NG), jnp.float32), (left_groups, right_groups))
    return total
```

```python
import math

import jax
import jax.numpy as jnp
import numpy as np
from jax import lax
from jax.sharding import PartitionSpec as P

AXES = ("pair", "ga")
CUTS = (512, 512, 512)
GAIN = 4.0

O, N, S, Z = (0, 0), (1, 0), (3, 0), (1, 1)
EARLY = ((O, O), (O, N), (O, S), (S, N))
LATE = ((O, Z), (Z, O), (Z, N), (Z, S))
PLAN = (
    ((0, 3, 2, 1), (1, 3, 0, 2), (0, 1, 1, 1)),
    ((2, 3, 1, 0), (1, 3, 2, 0), (1, 0, 0, 1)),
    ((2, 0, 3, 1), (3, 1, 2, 0), (1, 0, 1, 1)),
    ((1, 2, 0, 3), (2, 3, 1, 0), (0, 0, 1, 0)),
    ((1, 3, 0, 2), (0, 2, 1, 3), (0, 1, 0, 1)),
    ((3, 0, 2, 1), (1, 0, 3, 2), (1, 1, 0, 0)),
    ((1, 3, 2, 0), (2, 0, 3, 1), (1, 0, 1, 0)),
    ((0, 1, 3, 2), (0, 2, 3, 1), (1, 0, 0, 1)),
)


def index(x, y, z, core):
    x, y, z = x % 4, y % 4, z % 4
    return (4 * x + 2 * (z % 2) + core) * 8 + 4 * (z // 2) + y


def devices():
    for x in range(4):
        for y in range(4):
            for z in range(4):
                for core in range(2):
                    yield x, y, z, core


def shift(value, dx=0, dy=0, dz=0, swap=False):
    pairs = [
        (index(x, y, z, c), index(x + dx, y + dy, z + dz, 1 - c if swap else c))
        for x, y, z, c in devices()
    ]
    return lax.ppermute(value, AXES, pairs)


def swap_z_lo(value):
    pairs = [(index(x, y, z, c), index(x, y, z ^ 1, c)) for x, y, z, c in devices()]
    return lax.ppermute(value, AXES, pairs)


def to_owner(value):
    pairs = []
    for x, y, z, c in devices():
        early, late, keeper = PLAN[4 * (z // 2) + y]
        keeps = keeper[x] == z % 2
        row, col = EARLY[early[x]] if keeps else LATE[late[x]]
        row_y, row_hi = (y + row[0]) % 4, (z // 2 + row[1]) % 2
        block = 4 * ((z // 2 + col[1]) % 2) + (y + col[0]) % 4
        pairs.append(
            (index(x, y, z, c), index(block // 2, row_y, 2 * row_hi + block % 2, c))
        )
    return lax.ppermute(value, AXES, pairs)


def table():
    rows = []
    for pair in range(16):
        x, z_lo = pair // 4, pair // 2 % 2
        for ga in range(8):
            early, late, keeper = PLAN[ga]
            rows.append(
                [early[(x + d) % 4] for d in range(4)]
                + [late[(x + d) % 4] for d in range(4)]
                + [int(keeper[x] == z_lo)]
            )
    return np.array(rows, np.int32)


def lookup(bands, energy):
    levels = lax.broadcasted_iota(jnp.int32, (1, energy.shape[0]), 1)
    onehot = (bands[:, None] == levels).astype(jnp.float32)
    return jnp.sum(onehot * energy[None, :], axis=1)


def product(left, right):
    return lax.dot_general(
        left, right, (((0,), (0,)), ((), ())), preferred_element_type=jnp.float32
    )


def per_device(own, val_band, cond_band, val_energy, cond_energy):
    pairs_total = own.shape[0] * lax.axis_size("pair")
    pair, ga = lax.axis_index("pair"), lax.axis_index("ga")
    core = pair % 2
    plan = lax.dynamic_slice(jnp.asarray(table()), (pair * 8 + ga, 0), (1, 9))[0]

    gap = lookup(val_band, val_energy) - lookup(cond_band, cond_energy)
    weight = (4.0 * GAIN) / (gap * math.sqrt(pairs_total))

    def scale(block):
        return (weight[:, None] * block.astype(jnp.float32)).astype(jnp.bfloat16)

    north, south, across = [], [], []
    start = 0
    for size in CUTS:
        piece = own[start : start + size]
        start += size
        north.append(shift(piece, dy=-1))
        south.append(shift(piece, dy=1))
        across.append(shift(north[-1], dz=2))
    north, south, across = (jnp.concatenate(b, 0) for b in (north, south, across))
    half = own.shape[1] // 2

    def cols(block, side):
        return lax.dynamic_slice(block, (0, side * half), (block.shape[0], half))

    def stage(products):
        theirs = [product(left, cols(right, 1 - core)) for left, right in products]
        theirs = jnp.stack([t.astype(jnp.float16) for t in theirs])
        theirs = shift(theirs, swap=True)
        mine = jnp.stack([product(left, cols(right, core)) for left, right in products])
        return mine, theirs

    def over_x(mine, theirs, which):
        def pick(d):
            at = (which[d], 0, 0)
            size = (1,) + mine.shape[1:]
            return (
                lax.dynamic_slice(mine, at, size)[0]
                + lax.dynamic_slice(theirs, at, size)[0].astype(jnp.float32)
            )

        got = [shift(pick(d).astype(jnp.float16), dx=d) for d in (1, 3, 2)]
        return pick(0) + sum(g.astype(jnp.float32) for g in got)

    scaled = scale(own)
    early = stage(
        [(scaled, own), (scaled, north), (scaled, south), (scale(south), north)]
    )
    early = over_x(*early, plan[:4])
    far = scale(across)
    late = stage([(scaled, across), (far, own), (far, north), (far, south)])
    late = over_x(*late, plan[4:8])

    keeps = plan[8] == 1
    kept = jnp.where(keeps, early, late)
    got = swap_z_lo(jnp.where(keeps, late, early).astype(jnp.float16))
    total = kept + got.astype(jnp.float32)
    total = to_owner(total.astype(jnp.float16))
    return total.astype(jnp.float32) * (1.0 / GAIN)


def solution(mesh):
    placed = (P("pair", "ga"), P("pair"), P("pair"), P(), P())
    return jax.shard_map(
        per_device, mesh=mesh, in_specs=placed, out_specs=P("ga", "pair"), check_vma=False
    )
```

```python
import math

import jax
import jax.numpy as jnp
import numpy as np
from jax import lax
from jax.sharding import PartitionSpec as P


AXES = ("pair", "ga")
CUTS = (384, 384, 384, 384)
GAIN = 4.0

O, N, S, Z = (0, 0), (1, 0), (3, 0), (1, 1)
EARLY = ((O, O), (O, N), (O, S), (S, N))
LATE = ((O, Z), (Z, O), (Z, N), (Z, S))
PLAN = (
    ((0, 3, 2, 1), (1, 3, 0, 2), (0, 1, 1, 1)),
    ((2, 3, 1, 0), (1, 3, 2, 0), (1, 0, 0, 1)),
    ((2, 0, 3, 1), (3, 1, 2, 0), (1, 0, 1, 1)),
    ((1, 2, 0, 3), (2, 3, 1, 0), (0, 0, 1, 0)),
    ((1, 3, 0, 2), (0, 2, 1, 3), (0, 1, 0, 1)),
    ((3, 0, 2, 1), (1, 0, 3, 2), (1, 1, 0, 0)),
    ((1, 3, 2, 0), (2, 0, 3, 1), (1, 0, 1, 0)),
    ((0, 1, 3, 2), (0, 2, 3, 1), (1, 0, 0, 1)),
)


def index(x, y, z, core):
    x, y, z = x % 4, y % 4, z % 4
    return (4 * x + 2 * (z % 2) + core) * 8 + 4 * (z // 2) + y


def devices():
    for x in range(4):
        for y in range(4):
            for z in range(4):
                for core in range(2):
                    yield x, y, z, core


def shift(value, dx=0, dy=0, dz=0, swap=False):
    pairs = [
        (index(x, y, z, c), index(x + dx, y + dy, z + dz, 1 - c if swap else c))
        for x, y, z, c in devices()
    ]
    return lax.ppermute(value, AXES, pairs)


def swap_z_lo(value):
    pairs = [(index(x, y, z, c), index(x, y, z ^ 1, c)) for x, y, z, c in devices()]
    return lax.ppermute(value, AXES, pairs)


def to_owner(value):
    pairs = []
    for x, y, z, c in devices():
        early, late, keeper = PLAN[4 * (z // 2) + y]
        keeps = keeper[x] == z % 2
        row, col = EARLY[early[x]] if keeps else LATE[late[x]]
        row_y, row_hi = (y + row[0]) % 4, (z // 2 + row[1]) % 2
        block = 4 * ((z // 2 + col[1]) % 2) + (y + col[0]) % 4
        pairs.append(
            (index(x, y, z, c), index(block // 2, row_y, 2 * row_hi + block % 2, c))
        )
    return lax.ppermute(value, AXES, pairs)


def table():
    rows = []
    for pair in range(16):
        x, z_lo = pair // 4, pair // 2 % 2
        for ga in range(8):
            early, late, keeper = PLAN[ga]
            rows.append(
                [early[(x + d) % 4] for d in range(4)]
                + [late[(x + d) % 4] for d in range(4)]
                + [int(keeper[x] == z_lo)]
            )
    return np.array(rows, np.int32)


def lookup(bands, energy):
    levels = lax.broadcasted_iota(jnp.int32, (1, energy.shape[0]), 1)
    onehot = (bands[:, None] == levels).astype(jnp.float32)
    return jnp.sum(onehot * energy[None, :], axis=1)


def product(left, right):
    return lax.dot_general(
        left, right, (((0,), (0,)), ((), ())), preferred_element_type=jnp.float32
    )


def body(own, val_band, cond_band, val_energy, cond_energy):
    pairs_total = own.shape[0] * lax.axis_size("pair")
    pair, ga = lax.axis_index("pair"), lax.axis_index("ga")
    core = pair % 2
    plan = lax.dynamic_slice(jnp.asarray(table()), (pair * 8 + ga, 0), (1, 9))[0]
    half = own.shape[1] // 2
    starts = np.cumsum((0,) + CUTS)

    def rows(block, k):
        return block[starts[k] : starts[k + 1]]

    norths, farther = [], []
    for k in range(len(CUTS)):
        norths.append(shift(rows(own, k), dy=-1))
        if k == 0:
            south = shift(own, dy=1)
    for k in range(len(CUTS)):
        farther.append(shift(norths[k], dz=2))

    gap = lookup(val_band, val_energy) - lookup(cond_band, cond_energy)
    weight = (4.0 * GAIN) / (gap * math.sqrt(pairs_total))

    def scale(block, weight):
        return (weight[:, None] * block.astype(jnp.float32)).astype(jnp.bfloat16)

    def cols(block, side):
        return lax.dynamic_slice(block, (0, side * half), (block.shape[0], half))

    def swap(products):
        theirs = [product(left, cols(right, 1 - core)) for left, right in products]
        theirs = jnp.stack([t.astype(jnp.float16) for t in theirs])
        theirs = shift(theirs, swap=True)
        mine = jnp.stack([product(left, cols(right, core)) for left, right in products])
        return mine, theirs

    def over_x(mine, theirs, which):
        def pick(d):
            at = (which[d], 0, 0)
            size = (1,) + mine.shape[1:]
            return (
                lax.dynamic_slice(mine, at, size)[0]
                + lax.dynamic_slice(theirs, at, size)[0].astype(jnp.float32)
            )

        got = []
        for d in (1, 3, 2):
            got.append(shift(pick(d).astype(jnp.float16), dx=d))
        return pick(0), got

    north = jnp.concatenate(norths, 0)
    scaled = scale(own, weight)
    left = [scaled, scaled, scaled, scale(south, weight)]
    early = swap(list(zip(left, [own, north, south, north])))
    early, early_got = over_x(*early, plan[:4])

    far = jnp.concatenate(farther, 0)
    scaled_far = scale(far, weight)
    left = [scaled, scaled_far, scaled_far, scaled_far]
    late = swap(list(zip(left, [far, own, north, south])))
    late, late_got = over_x(*late, plan[4:8])

    early = early + sum(g.astype(jnp.float32) for g in early_got)
    late = late + sum(g.astype(jnp.float32) for g in late_got)
    keeps = plan[8] == 1
    kept = jnp.where(keeps, early, late)
    got = swap_z_lo(jnp.where(keeps, late, early).astype(jnp.float16))
    total = kept + got.astype(jnp.float32)
    total = to_owner(total.astype(jnp.float16))
    return total.astype(jnp.float32) * (1.0 / GAIN)


def solution(mesh):
    placed = (P("pair", "ga"), P("pair"), P("pair"), P(), P())
    return jax.shard_map(
        body, mesh=mesh, in_specs=placed, out_specs=P("ga", "pair"), check_vma=False
    )
```

```python
import math

import jax
import jax.numpy as jnp
import numpy as np
from jax import lax
from jax.experimental import pallas as pl
from jax.experimental.pallas import tpu as pltpu
from jax.sharding import PartitionSpec as P


AXES = ("pair", "ga")
CUTS = (384,) * 4
GAIN = 4.0

O, N, S, Z = (0, 0), (1, 0), (3, 0), (1, 1)
EARLY = ((O, O), (O, N), (O, S), (S, N))
LATE = ((O, Z), (Z, O), (Z, N), (S, Z))
PLAN = (
    ((3, 0, 2, 1), (1, 0, 3, 2), (0, 0, 1, 1)),
    ((2, 3, 1, 0), (1, 2, 3, 0), (1, 0, 0, 1)),
    ((1, 0, 3, 2), (3, 1, 2, 0), (0, 0, 1, 1)),
    ((1, 2, 0, 3), (2, 1, 3, 0), (0, 0, 1, 0)),
    ((2, 3, 1, 0), (0, 1, 2, 3), (0, 0, 1, 0)),
    ((1, 2, 0, 3), (3, 0, 1, 2), (1, 1, 1, 0)),
    ((1, 0, 2, 3), (0, 3, 1, 2), (1, 0, 0, 1)),
    ((0, 3, 1, 2), (0, 3, 2, 1), (1, 1, 0, 1)),
)


def index(x, y, z, core):
    x, y, z = x % 4, y % 4, z % 4
    return (4 * x + 2 * (z % 2) + core) * 8 + 4 * (z // 2) + y


def devices():
    for x in range(4):
        for y in range(4):
            for z in range(4):
                for core in range(2):
                    yield x, y, z, core


def shift(value, dx=0, dy=0, dz=0, swap=False):
    pairs = [
        (index(x, y, z, c), index(x + dx, y + dy, z + dz, 1 - c if swap else c))
        for x, y, z, c in devices()
    ]
    return lax.ppermute(value, AXES, pairs)


def swap_z_lo(value):
    pairs = [(index(x, y, z, c), index(x, y, z ^ 1, c)) for x, y, z, c in devices()]
    return lax.ppermute(value, AXES, pairs)


def to_owner(value):
    pairs = []
    for x, y, z, c in devices():
        early, late, keeper = PLAN[4 * (z // 2) + y]
        keeps = keeper[x] == z % 2
        row, col = EARLY[early[x]] if keeps else LATE[late[x]]
        row_y, row_hi = (y + row[0]) % 4, (z // 2 + row[1]) % 2
        block = 4 * ((z // 2 + col[1]) % 2) + (y + col[0]) % 4
        pairs.append(
            (index(x, y, z, c), index(block // 2, row_y, 2 * row_hi + block % 2, c))
        )
    return lax.ppermute(value, AXES, pairs)


def planned(pair, ga):
    x, z_lo = pair >> 2, (pair >> 1) & 1
    word = jnp.int32(0)
    for k, (early, late, keeper) in enumerate(PLAN):
        code = sum(v << 2 * i for i, v in enumerate(early + late))
        code += sum(v << 16 + i for i, v in enumerate(keeper))
        word = jnp.where(ga == k, code, word)

    def entry(d, base):
        return (word >> (2 * ((x + d) & 3) + base)) & 3

    early, late = ([entry(d, base) for d in range(4)] for base in (0, 8))
    return early, late, ((word >> (16 + x)) & 1) == z_lo


def lookup(bands, energy):
    levels = lax.broadcasted_iota(jnp.int32, (1, energy.shape[0]), 1)
    onehot = (bands[:, None] == levels).astype(jnp.float32)
    return jnp.sum(onehot * energy[None, :], axis=1)


def placing(which):
    return [sum(jnp.where(w == s, d, 0) for d, w in enumerate(which)) for s in range(4)]


def chunk(k):
    return slice(sum(CUTS[:k]), sum(CUTS[: k + 1]))


def fetch(sources, targets, sems):
    copies = [
        pltpu.make_async_copy(s, t, sems.at[i])
        for i, (s, t) in enumerate(zip(sources, targets))
    ]
    for copy in copies:
        copy.start()
    return copies


def matmul(left, right):
    return jnp.dot(left, right, preferred_element_type=jnp.float32)


def put(total, at, core, theirs, mine):
    low, high = total[:, : total.shape[1] // 2], total[:, total.shape[1] // 2 :]
    theirs[at] = jnp.where(core == 0, high, low)
    mine[at] = jnp.where(core == 0, low, high)


def scaled_transpose(weight, block):
    return (weight * block.astype(jnp.float32)).astype(jnp.bfloat16).T


COUNT = len(CUTS)


def early_kernel(*refs):
    sources, refs = refs[: 2 * COUNT + 3], refs[2 * COUNT + 3 :]
    theirs, mine, south_t = refs[:3]
    held, sems = refs[3:-1], refs[-1]
    copies = fetch(sources, held, sems)
    weight, own_t, own = held[:3]
    north, south = held[3 : 3 + COUNT], held[3 + COUNT :]
    pair, ga = lax.axis_index("pair"), lax.axis_index("ga")
    core, at = pair & 1, placing(planned(pair, ga)[0])
    for copy in copies[:3]:
        copy.wait()
    put(matmul(own_t[...], own[...]), at[0], core, theirs, mine)
    for copy in copies[3 : 3 + COUNT]:
        copy.wait()
    total = sum(matmul(own_t[:, chunk(k)], north[k][...]) for k in range(COUNT))
    put(total, at[1], core, theirs, mine)
    for copy in copies[3 + COUNT :]:
        copy.wait()
    total = sum(matmul(own_t[:, chunk(k)], south[k][...]) for k in range(COUNT))
    put(total, at[2], core, theirs, mine)
    for k in range(COUNT):
        south_t[:, chunk(k)] = scaled_transpose(weight[chunk(k), :], south[k][...])
    total = sum(matmul(south_t[:, chunk(k)], north[k][...]) for k in range(COUNT))
    put(total, at[3], core, theirs, mine)


def late_kernel(*refs):
    sources, refs = refs[: 2 * COUNT + 4], refs[2 * COUNT + 4 :]
    theirs, mine = refs[:2]
    held, far_t, sems = refs[2:-2], refs[-2], refs[-1]
    copies = fetch(sources, held, sems)
    weight, own_t, own, south_t = held[:4]
    north, far = held[4 : 4 + COUNT], held[4 + COUNT :]
    pair, ga = lax.axis_index("pair"), lax.axis_index("ga")
    core, at = pair & 1, placing(planned(pair, ga)[1])
    for copy in copies:
        copy.wait()
    total = sum(matmul(own_t[:, chunk(k)], far[k][...]) for k in range(COUNT))
    put(total, at[0], core, theirs, mine)
    for k in range(COUNT):
        far_t[:, chunk(k)] = scaled_transpose(weight[chunk(k), :], far[k][...])
    put(matmul(far_t[...], own[...]), at[1], core, theirs, mine)
    total = sum(matmul(far_t[:, chunk(k)], north[k][...]) for k in range(COUNT))
    put(total, at[2], core, theirs, mine)
    total = sum(matmul(south_t[:, chunk(k)], far[k][...]) for k in range(COUNT))
    put(total, at[3], core, theirs, mine)


def run_kernel(kernel, sources, outs, scratch):
    held = [pltpu.VMEM(s.shape, s.dtype) for s in sources]
    wide = sources[1].shape
    return pl.pallas_call(
        kernel,
        out_shape=outs,
        in_specs=[pl.BlockSpec(memory_space=pl.ANY)] * len(sources),
        out_specs=[pl.BlockSpec(memory_space=pltpu.VMEM)] * len(outs),
        scratch_shapes=[*held, *scratch, pltpu.SemaphoreType.DMA((len(sources),))],
        compiler_params=pltpu.CompilerParams(vmem_limit_bytes=32 * 2**20),
        cost_estimate=pl.CostEstimate(
            flops=8 * wide[0] * wide[0] * wide[1], bytes_accessed=2**23, transcendentals=0
        ),
    )(*sources)


def body(own, val_band, cond_band, val_energy, cond_energy):
    pairs_total = own.shape[0] * lax.axis_size("pair")
    pair, ga = lax.axis_index("pair"), lax.axis_index("ga")
    starts = np.cumsum((0,) + CUTS)

    def rows(block, k):
        return block[starts[k] : starts[k + 1]]

    norths, souths, farther = [], [], []
    first = rows(own, 0)
    rest = lax.optimization_barrier((own, first))[0]
    for k in range(len(CUTS)):
        piece = rows(rest, k) if k else first
        norths.append(shift(piece, dy=-1))
        souths.append(shift(piece, dy=1))
        farther.append(shift(norths[k], dz=2))

    gap = lookup(val_band, val_energy) - lookup(cond_band, cond_energy)
    weight = (4.0 * GAIN) / (gap * math.sqrt(pairs_total))

    size = own.shape[1]
    half = jax.ShapeDtypeStruct((4, size, size // 2), jnp.float32)
    flipped = jax.ShapeDtypeStruct(own.shape[::-1], own.dtype)

    def over_x(theirs, mine):
        theirs = shift(theirs.astype(jnp.float16), swap=True)

        def joined(d):
            return mine[d] + theirs[d].astype(jnp.float32)

        got, sent = [], [joined(d).astype(jnp.float16) for d in (1, 3, 2)]
        for d, value in zip((1, 3, 2), sent):
            got.append(shift(value, dx=d))
        return joined(0), got, sent

    column = weight[:, None]
    own_t = (column * own.astype(jnp.float32)).astype(jnp.bfloat16).T
    column, own_t = lax.optimization_barrier((column, own_t))

    *products, south_t = run_kernel(
        early_kernel,
        [column, own_t, own, *norths, *souths],
        [half, half, flipped],
        [],
    )
    early, early_got, _ = over_x(*products)

    products = run_kernel(
        late_kernel,
        [column, own_t, own, south_t, *norths, *farther],
        [half, half],
        [pltpu.VMEM(flipped.shape, flipped.dtype)],
    )
    late, late_got, _ = over_x(*products)

    early = early + sum(g.astype(jnp.float32) for g in early_got)
    early = lax.optimization_barrier(early)
    late = late + sum(g.astype(jnp.float32) for g in late_got)
    keeps = planned(pair, ga)[2]
    kept = jnp.where(keeps, early, late)
    got = swap_z_lo(jnp.where(keeps, late, early).astype(jnp.float16))
    total = kept + got.astype(jnp.float32)
    total = to_owner(total.astype(jnp.float16))
    return total.astype(jnp.float32) * (1.0 / GAIN)


def solution(mesh):
    placed = (P("pair", "ga"), P("pair"), P("pair"), P(), P())
    return jax.shard_map(
        body, mesh=mesh, in_specs=placed, out_specs=P("ga", "pair"), check_vma=False
    )
```

```python
import functools
import math

import jax
import jax.numpy as jnp
import numpy as np
from jax import lax
from jax.experimental import pallas as pl
from jax.experimental.pallas import tpu as pltpu
from jax.sharding import PartitionSpec as P


AXES = ("pair", "ga")
CUTS = (384,) * 4
GAIN = 4.0

O, N, S, Z = (0, 0), (1, 0), (3, 0), (1, 1)
EARLY = ((O, O), (O, N), (O, S), (S, N))
LATE = ((O, Z), (Z, O), (Z, N), (S, Z))
PLAN = (
    ((3, 0, 2, 1), (1, 0, 3, 2), (0, 0, 1, 1)),
    ((2, 3, 1, 0), (1, 2, 3, 0), (1, 0, 0, 1)),
    ((1, 0, 3, 2), (3, 1, 2, 0), (0, 0, 1, 1)),
    ((1, 2, 0, 3), (2, 1, 3, 0), (0, 0, 1, 0)),
    ((2, 3, 1, 0), (0, 1, 2, 3), (0, 0, 1, 0)),
    ((1, 2, 0, 3), (3, 0, 1, 2), (1, 1, 1, 0)),
    ((1, 0, 2, 3), (0, 3, 1, 2), (1, 0, 0, 1)),
    ((0, 3, 1, 2), (0, 3, 2, 1), (1, 1, 0, 1)),
)


def index(x, y, z, core):
    x, y, z = x % 4, y % 4, z % 4
    return (4 * x + 2 * (z % 2) + core) * 8 + 4 * (z // 2) + y


def devices():
    for x in range(4):
        for y in range(4):
            for z in range(4):
                for core in range(2):
                    yield x, y, z, core


def shift(value, dx=0, dy=0, dz=0, swap=False):
    pairs = [
        (index(x, y, z, c), index(x + dx, y + dy, z + dz, 1 - c if swap else c))
        for x, y, z, c in devices()
    ]
    return lax.ppermute(value, AXES, pairs)


def swap_z_lo(value):
    pairs = [(index(x, y, z, c), index(x, y, z ^ 1, c)) for x, y, z, c in devices()]
    return lax.ppermute(value, AXES, pairs)


def to_owner(value):
    pairs = []
    for x, y, z, c in devices():
        early, late, keeper = PLAN[4 * (z // 2) + y]
        keeps = keeper[x] == z % 2
        row, col = EARLY[early[x]] if keeps else LATE[late[x]]
        row_y, row_hi = (y + row[0]) % 4, (z // 2 + row[1]) % 2
        block = 4 * ((z // 2 + col[1]) % 2) + (y + col[0]) % 4
        pairs.append(
            (index(x, y, z, c), index(block // 2, row_y, 2 * row_hi + block % 2, c))
        )
    return lax.ppermute(value, AXES, pairs)


def planned(pair, ga):
    x, z_lo = pair >> 2, (pair >> 1) & 1
    word = jnp.int32(0)
    for k, (early, late, keeper) in enumerate(PLAN):
        code = sum(v << 2 * i for i, v in enumerate(early + late))
        code += sum(v << 16 + i for i, v in enumerate(keeper))
        word = jnp.where(ga == k, code, word)

    def entry(d, base):
        return (word >> (2 * ((x + d) & 3) + base)) & 3

    early, late = ([entry(d, base) for d in range(4)] for base in (0, 8))
    return early, late, ((word >> (16 + x)) & 1) == z_lo


def lookup(bands, energy):
    levels = lax.broadcasted_iota(jnp.int32, (1, energy.shape[0]), 1)
    onehot = (bands[:, None] == levels).astype(jnp.float32)
    return jnp.sum(onehot * energy[None, :], axis=1)


def placing(which):
    return [sum(jnp.where(w == s, d, 0) for d, w in enumerate(which)) for s in range(4)]


def chunk(k):
    return slice(sum(CUTS[:k]), sum(CUTS[: k + 1]))


COUNT = len(CUTS)
SPLIT = 2


def stage_kernel(late, lo, hi, n_in, *refs):
    first, last = lo == 0, hi == COUNT
    sources, refs = refs[:n_in], refs[n_in:]
    n_out = (2 if last else 1) + (not late)
    outs, (row, own_t, own, north, far, *rest, sems) = refs[:n_out], refs[n_out:]
    rows = slice(chunk(lo).start, chunk(hi - 1).stop)
    spans = [slice(chunk(k).start - rows.start, chunk(k).stop - rows.start) for k in range(lo, hi)]
    pairs = [
        (sources[0].at[:, rows], row),
        (sources[1].at[:, rows], own_t),
        (sources[2].at[rows, :], own),
        *((s, north.at[c]) for s, c in zip(sources[3:], spans)),
        *((s, far.at[c]) for s, c in zip(sources[3 + hi - lo :], spans)),
    ]
    extra = sources[len(pairs) :]
    if late:
        south_t, flipped = rest
        edge = chunk(SPLIT).start
        pairs += [(extra[0], south_t.at[:, :edge]), (extra[1], south_t.at[:, edge:])]
    else:
        flipped = outs[-1]
        pairs += zip(extra, rest)
    copies = [
        pltpu.make_async_copy(s, t, sems.at[i]) for i, (s, t) in enumerate(pairs)
    ]
    for copy in copies:
        copy.start()
    pair, ga = lax.axis_index("pair"), lax.axis_index("ga")
    core, at = pair & 1, placing(planned(pair, ga)[int(late)])
    half = own.shape[1] // 2

    def put(i, left, right):
        total = jnp.dot(left[...], right[...], preferred_element_type=jnp.float32)
        if not first:
            total = total + rest[0][i]
        if last:
            low, high = total[:, :half], total[:, half:]
            outs[0][at[i]] = jnp.where(core == 0, high, low)
            outs[1][at[i]] = jnp.where(core == 0, low, high)
        else:
            outs[0][i] = total

    for copy in copies:
        copy.wait()
    if late:
        put(0, own_t, far)
    else:
        put(0, own_t, own)
        put(1, own_t, north)
        put(2, own_t, far)
    flipped[...] = (row[...] * far[...].T.astype(jnp.float32)).astype(flipped.dtype)
    if late:
        put(1, flipped, own)
        put(2, flipped, north)
        put(3, south_t, far)
    else:
        put(3, flipped, north)


def run_stage(late, lo, hi, sources):
    size, _ = sources[1].shape
    rows = sum(CUTS[lo:hi])
    tall, wide = ((rows, size), jnp.bfloat16), ((size, rows), jnp.bfloat16)
    held = [((1, rows), jnp.float32), wide, tall, tall, tall]
    outs = [((4, size, size), jnp.float32)]
    if late:
        held += [wide, wide]
    elif lo:
        held += outs
    if hi == COUNT:
        outs = [((4, size, size // 2), jnp.float32)] * 2
    if not late:
        outs.append(wide)
    return pl.pallas_call(
        functools.partial(stage_kernel, late, lo, hi, len(sources)),
        out_shape=[jax.ShapeDtypeStruct(*o) for o in outs],
        in_specs=[pl.BlockSpec(memory_space=pl.ANY)] * len(sources),
        out_specs=[pl.BlockSpec(memory_space=pltpu.VMEM)] * len(outs),
        scratch_shapes=[
            *(pltpu.VMEM(*h) for h in held),
            pltpu.SemaphoreType.DMA((len(sources),)),
        ],
        compiler_params=pltpu.CompilerParams(vmem_limit_bytes=28 * 2**20),
        cost_estimate=pl.CostEstimate(
            flops=8 * size * size * rows, bytes_accessed=2**23, transcendentals=0
        ),
    )(*sources)


def body(own, val_band, cond_band, val_energy, cond_energy):
    pairs_total = own.shape[0] * lax.axis_size("pair")
    pair, ga = lax.axis_index("pair"), lax.axis_index("ga")
    starts = np.cumsum((0,) + CUTS)

    def rows(block, k):
        return block[starts[k] : starts[k + 1]]

    norths, souths, farther = [], [], []
    first = rows(own, 0)
    rest = lax.optimization_barrier((own, first))[0]
    for k in range(len(CUTS)):
        piece = rows(rest, k) if k else first
        norths.append(shift(piece, dy=-1))
        souths.append(shift(piece, dy=1))
        farther.append(shift(norths[k], dz=2))

    def over_x(theirs, mine):
        theirs = shift(theirs.astype(jnp.float16), swap=True)
        joined = [mine[d] + theirs[d].astype(jnp.float32) for d in range(4)]
        kept, *sent = lax.optimization_barrier(
            [joined[0]] + [joined[d].astype(jnp.float16) for d in (1, 3, 2)]
        )
        got = []
        for d, value in zip((1, 3, 2), sent):
            got.append(shift(value, dx=d))
        return kept, got

    gap = lookup(val_band, val_energy) - lookup(cond_band, cond_energy)
    weight = (4.0 * GAIN) / (gap * math.sqrt(pairs_total))
    row = weight[None, :]
    own_t = (row * own.T.astype(jnp.float32)).astype(jnp.bfloat16)
    row, own_t = lax.optimization_barrier((row, own_t))
    base = [row, own_t, own]
    one, two = slice(0, SPLIT), slice(SPLIT, COUNT)

    early_sum, south_a = run_stage(False, 0, SPLIT, base + norths[one] + souths[one])
    *early, south_b = run_stage(
        False, SPLIT, COUNT, base + norths[two] + souths[two] + [early_sum]
    )
    early, early_got = over_x(*early)
    late = run_stage(
        True, 0, COUNT, base + norths + farther + [south_a, south_b]
    )
    late, late_got = over_x(*late)

    early = early + sum(g.astype(jnp.float32) for g in early_got)
    early = lax.optimization_barrier(early)
    late = late + sum(g.astype(jnp.float32) for g in late_got)
    keeps = planned(pair, ga)[2]
    kept = jnp.where(keeps, early, late)
    got = swap_z_lo(jnp.where(keeps, late, early).astype(jnp.float16))
    total = kept + got.astype(jnp.float32)
    total = to_owner(total.astype(jnp.float16))
    return total.astype(jnp.float32) * (1.0 / GAIN)


def solution(mesh):
    placed = (P("pair", "ga"), P("pair"), P("pair"), P(), P())
    return jax.shard_map(
        body, mesh=mesh, in_specs=placed, out_specs=P("ga", "pair"), check_vma=False
    )
```

```python
import functools
import math

import jax
import jax.numpy as jnp
import numpy as np
from jax import lax
from jax.experimental import pallas as pl
from jax.experimental.pallas import tpu as pltpu
from jax.sharding import PartitionSpec as P


AXES = ("pair", "ga")
CUTS = (384,) * 4
GAIN = 4.0

O, N, S, Z = (0, 0), (1, 0), (3, 0), (1, 1)
EARLY = ((O, O), (O, N), (O, S), (S, N))
LATE = ((O, Z), (Z, O), (Z, N), (S, Z))
PLAN = (
    ((3, 0, 2, 1), (2, 1, 0, 3), (1, 0, 1, 0)),
    ((2, 3, 1, 0), (1, 2, 0, 3), (1, 0, 0, 1)),
    ((0, 3, 1, 2), (0, 1, 2, 3), (0, 0, 1, 0)),
    ((3, 2, 0, 1), (2, 1, 3, 0), (0, 1, 1, 1)),
    ((2, 1, 3, 0), (3, 0, 2, 1), (1, 1, 1, 0)),
    ((1, 0, 2, 3), (0, 3, 1, 2), (1, 1, 1, 0)),
    ((1, 2, 0, 3), (2, 3, 0, 1), (1, 0, 0, 0)),
    ((0, 1, 3, 2), (3, 0, 2, 1), (1, 1, 0, 1)),
)


def index(x, y, z, core):
    x, y, z = x % 4, y % 4, z % 4
    return (4 * x + 2 * (z % 2) + core) * 8 + 4 * (z // 2) + y


def devices():
    for x in range(4):
        for y in range(4):
            for z in range(4):
                for core in range(2):
                    yield x, y, z, core


def shift(value, dx=0, dy=0, dz=0, swap=False):
    pairs = [
        (index(x, y, z, c), index(x + dx, y + dy, z + dz, 1 - c if swap else c))
        for x, y, z, c in devices()
    ]
    return lax.ppermute(value, AXES, pairs)


def swap_z_lo(value):
    pairs = [(index(x, y, z, c), index(x, y, z ^ 1, c)) for x, y, z, c in devices()]
    return lax.ppermute(value, AXES, pairs)


def to_owner(value):
    pairs = []
    for x, y, z, c in devices():
        early, late, keeper = PLAN[4 * (z // 2) + y]
        keeps = keeper[x] == z % 2
        row, col = EARLY[early[x]] if keeps else LATE[late[x]]
        row_y, row_hi = (y + row[0]) % 4, (z // 2 + row[1]) % 2
        block = 4 * ((z // 2 + col[1]) % 2) + (y + col[0]) % 4
        pairs.append(
            (index(x, y, z, c), index(block // 2, row_y, 2 * row_hi + block % 2, c))
        )
    return lax.ppermute(value, AXES, pairs)


def planned(pair, ga):
    x, z_lo = pair >> 2, (pair >> 1) & 1
    word = jnp.int32(0)
    for k, (early, late, keeper) in enumerate(PLAN):
        code = sum(v << 2 * i for i, v in enumerate(early + late))
        code += sum(v << 16 + i for i, v in enumerate(keeper))
        word = jnp.where(ga == k, code, word)

    def entry(d, base):
        return (word >> (2 * ((x + d) & 3) + base)) & 3

    early, late = ([entry(d, base) for d in range(4)] for base in (0, 8))
    return early, late, ((word >> (16 + x)) & 1) == z_lo


def lookup(bands, energy):
    levels = lax.broadcasted_iota(jnp.int32, (1, energy.shape[0]), 1)
    onehot = (bands[:, None] == levels).astype(jnp.float32)
    return jnp.sum(onehot * energy[None, :], axis=1)


def placing(which):
    return [sum(jnp.where(w == s, d, 0) for d, w in enumerate(which)) for s in range(4)]


def chunk(k):
    return slice(sum(CUTS[:k]), sum(CUTS[: k + 1]))


COUNT = len(CUTS)
TAIL = (256, 512)
SPLIT = 2


def stage_kernel(late, lo, hi, n_in, *refs):
    first, last = lo == 0, hi == COUNT
    sources, refs = refs[:n_in], refs[n_in:]
    n_out = (2 if last else 1) + (not late)
    outs, (row, own_t, own, north, far, *rest, sems) = refs[:n_out], refs[n_out:]
    rows = slice(chunk(lo).start, chunk(hi - 1).stop)
    spans = [slice(chunk(k).start - rows.start, chunk(k).stop - rows.start) for k in range(lo, hi)]
    pairs = [
        (sources[0].at[:, rows], row),
        (sources[1].at[:, rows], own_t),
        (sources[2].at[rows, :], own),
        *((s, north.at[c]) for s, c in zip(sources[3:], spans)),
        *((s, far.at[c]) for s, c in zip(sources[3 + hi - lo :], spans)),
    ]
    extra = sources[len(pairs) :]
    if late:
        south_t, flipped = rest
        edge = chunk(SPLIT).start
        pairs += [(extra[0], south_t.at[:, :edge]), (extra[1], south_t.at[:, edge:])]
    else:
        flipped = outs[-1]
        pairs += zip(extra, rest)
    copies = [
        pltpu.make_async_copy(s, t, sems.at[i]) for i, (s, t) in enumerate(pairs)
    ]
    for copy in copies:
        copy.start()
    pair, ga = lax.axis_index("pair"), lax.axis_index("ga")
    core, at = pair & 1, placing(planned(pair, ga)[int(late)])
    half = own.shape[1] // 2

    def put(i, left, right):
        total = jnp.dot(left[...], right[...], preferred_element_type=jnp.float32)
        if not first:
            total = total + rest[0][i]
        if last:
            low, high = total[:, :half], total[:, half:]
            outs[0][at[i]] = jnp.where(core == 0, high, low)
            outs[1][at[i]] = jnp.where(core == 0, low, high)
        else:
            outs[0][i] = total

    for copy in copies:
        copy.wait()
    if late:
        put(0, own_t, far)
    else:
        put(0, own_t, own)
        put(1, own_t, north)
        put(2, own_t, far)
    flipped[...] = (row[...] * far[...].T.astype(jnp.float32)).astype(flipped.dtype)
    if late:
        put(1, flipped, own)
        put(2, flipped, north)
        put(3, south_t, far)
    else:
        put(3, flipped, north)


def run_stage(late, lo, hi, sources):
    size, _ = sources[1].shape
    rows = sum(CUTS[lo:hi])
    tall, wide = ((rows, size), jnp.bfloat16), ((size, rows), jnp.bfloat16)
    held = [((1, rows), jnp.float32), wide, tall, tall, tall]
    outs = [((4, size, size), jnp.float32)]
    if late:
        held += [wide, wide]
    elif lo:
        held += outs
    if hi == COUNT:
        outs = [((4, size, size // 2), jnp.float32)] * 2
    if not late:
        outs.append(wide)
    return pl.pallas_call(
        functools.partial(stage_kernel, late, lo, hi, len(sources)),
        out_shape=[jax.ShapeDtypeStruct(*o) for o in outs],
        in_specs=[pl.BlockSpec(memory_space=pl.ANY)] * len(sources),
        out_specs=[pl.BlockSpec(memory_space=pltpu.VMEM)] * len(outs),
        scratch_shapes=[
            *(pltpu.VMEM(*h) for h in held),
            pltpu.SemaphoreType.DMA((len(sources),)),
        ],
        compiler_params=pltpu.CompilerParams(vmem_limit_bytes=28 * 2**20),
        cost_estimate=pl.CostEstimate(
            flops=8 * size * size * rows, bytes_accessed=2**23, transcendentals=0
        ),
    )(*sources)


def body(own, val_band, cond_band, val_energy, cond_energy):
    pairs_total = own.shape[0] * lax.axis_size("pair")
    pair, ga = lax.axis_index("pair"), lax.axis_index("ga")
    starts = np.cumsum((0,) + CUTS)

    def rows(block, k):
        return block[starts[k] : starts[k + 1]]

    norths, souths, farther = [], [], []
    first = rows(own, 0)
    rest = lax.optimization_barrier((own, first))[0]
    for k in range(len(CUTS)):
        piece = rows(rest, k) if k else first
        norths.append(shift(piece, dy=-1))
        souths.append(shift(piece, dy=1))
        farther.append(shift(norths[k], dz=2))

    def over_x(theirs, mine):
        theirs = shift(theirs.astype(jnp.float16), swap=True)
        joined = [mine[d] + theirs[d].astype(jnp.float32) for d in range(4)]
        kept, *sent = lax.optimization_barrier(
            [joined[0]] + [joined[d].astype(jnp.float16) for d in (1, 3, 2)]
        )
        got = []
        for d, value in zip((1, 3, 2), sent):
            got.append(shift(value, dx=d))
        return kept, got

    gap = lookup(val_band, val_energy) - lookup(cond_band, cond_energy)
    weight = (4.0 * GAIN) / (gap * math.sqrt(pairs_total))
    row = weight[None, :]
    own_t = (row * own.T.astype(jnp.float32)).astype(jnp.bfloat16)
    row, own_t = lax.optimization_barrier((row, own_t))
    base = [row, own_t, own]
    one, two = slice(0, SPLIT), slice(SPLIT, COUNT)

    early_sum, south_a = run_stage(False, 0, SPLIT, base + norths[one] + souths[one])
    *early, south_b = run_stage(
        False, SPLIT, COUNT, base + norths[two] + souths[two] + [early_sum]
    )
    early, early_got = over_x(*early)
    late = run_stage(
        True, 0, COUNT, base + norths + farther + [south_a, south_b]
    )
    late, late_got = over_x(*late)

    def sum_of(kept, got):
        return kept + sum(g.astype(jnp.float32) for g in got)

    early = lax.optimization_barrier(sum_of(early, early_got))
    late = sum_of(late, late_got)
    keeps = planned(pair, ga)[2]
    kept = jnp.where(keeps, early, late)
    sent = jnp.where(keeps, late, early).astype(jnp.float16)
    parts, edges, total = [], (0, *TAIL), None
    for h, part in enumerate(slice(u, v) for u, v in zip(edges, edges[1:])):
        got = swap_z_lo(sent[part])
        if h:
            got = lax.optimization_barrier((got, total))[0]
        total = (kept[part] + got.astype(jnp.float32)).astype(jnp.float16)
        parts.append(to_owner(total))
    return jnp.concatenate(parts, 0).astype(jnp.float32) * (1.0 / GAIN)


def solution(mesh):
    placed = (P("pair", "ga"), P("pair"), P("pair"), P(), P())
    return jax.shard_map(
        body, mesh=mesh, in_specs=placed, out_specs=P("ga", "pair"), check_vma=False
    )
```

```python
import functools
import math

import jax
import jax.numpy as jnp
import numpy as np
from jax import lax
from jax.experimental import pallas as pl
from jax.experimental.pallas import tpu as pltpu
from jax.sharding import PartitionSpec as P


AXES = ("pair", "ga")
CUTS = (384,) * 4
GAIN = 4.0

O, N, S, Z = (0, 0), (1, 0), (3, 0), (1, 1)
EARLY = ((O, O), (O, N), (O, S), (S, N))
LATE = ((O, Z), (Z, O), (Z, N), (S, Z))
PLAN = (
    ((3, 0, 2, 1), (2, 1, 0, 3), (1, 0, 1, 0)),
    ((2, 3, 1, 0), (1, 2, 0, 3), (1, 0, 0, 1)),
    ((0, 3, 1, 2), (0, 1, 2, 3), (0, 0, 1, 0)),
    ((3, 2, 0, 1), (2, 1, 3, 0), (0, 1, 1, 1)),
    ((2, 1, 3, 0), (3, 0, 2, 1), (1, 1, 1, 0)),
    ((1, 0, 2, 3), (0, 3, 1, 2), (1, 1, 1, 0)),
    ((1, 2, 0, 3), (2, 3, 0, 1), (1, 0, 0, 0)),
    ((0, 1, 3, 2), (3, 0, 2, 1), (1, 1, 0, 1)),
)


def index(x, y, z, core):
    x, y, z = x % 4, y % 4, z % 4
    return (4 * x + 2 * (z % 2) + core) * 8 + 4 * (z // 2) + y


def devices():
    for x in range(4):
        for y in range(4):
            for z in range(4):
                for core in range(2):
                    yield x, y, z, core


def shift(value, dx=0, dy=0, dz=0, swap=False):
    pairs = [
        (index(x, y, z, c), index(x + dx, y + dy, z + dz, 1 - c if swap else c))
        for x, y, z, c in devices()
    ]
    return lax.ppermute(value, AXES, pairs)


def swap_z_lo(value):
    pairs = [(index(x, y, z, c), index(x, y, z ^ 1, c)) for x, y, z, c in devices()]
    return lax.ppermute(value, AXES, pairs)


def to_owner(value):
    pairs = []
    for x, y, z, c in devices():
        early, late, keeper = PLAN[4 * (z // 2) + y]
        keeps = keeper[x] == z % 2
        row, col = EARLY[early[x]] if keeps else LATE[late[x]]
        row_y, row_hi = (y + row[0]) % 4, (z // 2 + row[1]) % 2
        block = 4 * ((z // 2 + col[1]) % 2) + (y + col[0]) % 4
        pairs.append(
            (index(x, y, z, c), index(block // 2, row_y, 2 * row_hi + block % 2, c))
        )
    return lax.ppermute(value, AXES, pairs)


def planned(pair, ga):
    x, z_lo = pair >> 2, (pair >> 1) & 1
    word = jnp.int32(0)
    for k, (early, late, keeper) in enumerate(PLAN):
        code = sum(v << 2 * i for i, v in enumerate(early + late))
        code += sum(v << 16 + i for i, v in enumerate(keeper))
        word = jnp.where(ga == k, code, word)

    def entry(d, base):
        return (word >> (2 * ((x + d) & 3) + base)) & 3

    early, late = ([entry(d, base) for d in range(4)] for base in (0, 8))
    return early, late, ((word >> (16 + x)) & 1) == z_lo


def lookup(bands, energy):
    levels = lax.broadcasted_iota(jnp.int32, (1, energy.shape[0]), 1)
    onehot = (bands[:, None] == levels).astype(jnp.float32)
    return jnp.sum(onehot * energy[None, :], axis=1)


def placing(which):
    return [sum(jnp.where(w == s, d, 0) for d, w in enumerate(which)) for s in range(4)]


def chunk(k):
    return slice(sum(CUTS[:k]), sum(CUTS[: k + 1]))


COUNT = len(CUTS)
TAIL = (256, 512)
SPLIT = 2


def stage_kernel(late, lo, hi, n_in, *refs):
    first, last = lo == 0, hi == COUNT
    sources, refs = refs[:n_in], refs[n_in:]
    n_out = (2 if last else 1) + (not late)
    outs, (row, own_t, own, north, far, *rest, sems) = refs[:n_out], refs[n_out:]
    rows = slice(chunk(lo).start, chunk(hi - 1).stop)
    spans = [slice(chunk(k).start - rows.start, chunk(k).stop - rows.start) for k in range(lo, hi)]
    pairs = [
        (sources[0].at[:, rows], row),
        (sources[1].at[:, rows], own_t),
        (sources[2].at[rows, :], own),
        *((s, north.at[c]) for s, c in zip(sources[3:], spans)),
        *((s, far.at[c]) for s, c in zip(sources[3 + hi - lo :], spans)),
    ]
    extra = sources[len(pairs) :]
    if late:
        left, flipped = own_t, rest[0]
        size, edge = own.shape[1], chunk(SPLIT).start
        pairs[1] = (sources[1], left.at[:size])
        pairs += [
            (extra[0], left.at[size:, :edge]),
            (extra[1], left.at[size:, edge:]),
        ]
    else:
        flipped = outs[-1]
        pairs += zip(extra, rest)
    copies = [
        pltpu.make_async_copy(s, t, sems.at[i]) for i, (s, t) in enumerate(pairs)
    ]
    for copy in copies:
        copy.start()
    pair, ga = lax.axis_index("pair"), lax.axis_index("ga")
    core, at = pair & 1, placing(planned(pair, ga)[int(late)])
    half = own.shape[1] // 2

    def put(i, left, right):
        keep(i, jnp.dot(left[...], right[...], preferred_element_type=jnp.float32))

    def keep(i, total):
        if not first:
            total = total + rest[0][i]
        if last:
            low, high = total[:, :half], total[:, half:]
            outs[0][at[i]] = jnp.where(core == 0, high, low)
            outs[1][at[i]] = jnp.where(core == 0, low, high)
        else:
            outs[0][i] = total

    for copy in copies:
        copy.wait()
    if late:
        total = jnp.dot(left[...], far[...], preferred_element_type=jnp.float32)
        size = own.shape[1]
        keep(0, total[:size])
        keep(3, total[size:])
    else:
        put(0, own_t, own)
        put(1, own_t, north)
        put(2, own_t, far)
    flipped[...] = (row[...] * far[...].T.astype(jnp.float32)).astype(flipped.dtype)
    if late:
        put(1, flipped, own)
        put(2, flipped, north)
    else:
        put(3, flipped, north)


def run_stage(late, lo, hi, sources):
    size, _ = sources[1].shape
    rows = sum(CUTS[lo:hi])
    tall, wide = ((rows, size), jnp.bfloat16), ((size, rows), jnp.bfloat16)
    held = [((1, rows), jnp.float32), wide, tall, tall, tall]
    outs = [((4, size, size), jnp.float32)]
    if late:
        held[1] = ((2 * size, rows), jnp.bfloat16)
        held.append(wide)
    elif lo:
        held += outs
    if hi == COUNT:
        outs = [((4, size, size // 2), jnp.float32)] * 2
    if not late:
        outs.append(wide)
    return pl.pallas_call(
        functools.partial(stage_kernel, late, lo, hi, len(sources)),
        out_shape=[jax.ShapeDtypeStruct(*o) for o in outs],
        in_specs=[pl.BlockSpec(memory_space=pl.ANY)] * len(sources),
        out_specs=[pl.BlockSpec(memory_space=pltpu.VMEM)] * len(outs),
        scratch_shapes=[
            *(pltpu.VMEM(*h) for h in held),
            pltpu.SemaphoreType.DMA((len(sources),)),
        ],
        compiler_params=pltpu.CompilerParams(vmem_limit_bytes=28 * 2**20),
        cost_estimate=pl.CostEstimate(
            flops=8 * size * size * rows, bytes_accessed=2**23, transcendentals=0
        ),
    )(*sources)


def body(own, val_band, cond_band, val_energy, cond_energy):
    pairs_total = own.shape[0] * lax.axis_size("pair")
    pair, ga = lax.axis_index("pair"), lax.axis_index("ga")
    starts = np.cumsum((0,) + CUTS)

    def rows(block, k):
        return block[starts[k] : starts[k + 1]]

    norths, souths, farther = [], [], []
    first = rows(own, 0)
    rest = lax.optimization_barrier((own, first))[0]
    for k in range(len(CUTS)):
        piece = rows(rest, k) if k else first
        norths.append(shift(piece, dy=-1))
        souths.append(shift(piece, dy=1))
        farther.append(shift(norths[k], dz=2))

    def over_x(theirs, mine, parts):
        theirs, mine = lax.optimization_barrier(
            (theirs.astype(jnp.float16), mine.astype(jnp.float16))
        )
        theirs = shift(theirs, swap=True)
        theirs, mine = theirs.astype(jnp.float32), mine.astype(jnp.float32)
        joined = [mine[d] + theirs[d] for d in range(4)]
        kept, *sent = lax.optimization_barrier(
            [joined[0]] + [joined[d].astype(jnp.float16) for d in (1, 3, 2)]
        )
        got = []
        for part in parts:
            got.append([])
            for d, value in zip((1, 3, 2), sent):
                got[-1].append(shift(value[part], dx=d))
        return kept, got

    gap = lookup(val_band, val_energy) - lookup(cond_band, cond_energy)
    weight = (4.0 * GAIN) / (gap * math.sqrt(pairs_total))
    row = weight[None, :]
    own_t = (row * own.T.astype(jnp.float32)).astype(jnp.bfloat16)
    row, own_t = lax.optimization_barrier((row, own_t))
    base = [row, own_t, own]
    tail = [slice(u, v) for u, v in zip((0, *TAIL), TAIL)]
    one, two = slice(0, SPLIT), slice(SPLIT, COUNT)

    early_sum, south_a = run_stage(False, 0, SPLIT, base + norths[one] + souths[one])
    *early, south_b = run_stage(
        False, SPLIT, COUNT, base + norths[two] + souths[two] + [early_sum]
    )
    early, early_got = over_x(*early, [slice(None)])
    late = run_stage(
        True, 0, COUNT, base + norths + farther + [south_a, south_b]
    )
    late, late_got = over_x(*late, tail)

    def sum_of(kept, got):
        return kept + sum(g.astype(jnp.float32) for g in got)

    def after(value, other):
        return value if other is None else lax.optimization_barrier((value, other))[0]

    early = lax.optimization_barrier(sum_of(early, early_got[0]))
    keeps = planned(pair, ga)[2]
    pieces, sent, total = [], None, None
    for h, part in enumerate(tail):
        whole = sum_of(late[part], after(late_got[h], sent))
        kept = jnp.where(keeps, early[part], whole)
        sent = jnp.where(keeps, whole, early[part]).astype(jnp.float16)
        pieces.append((kept, swap_z_lo(sent)))
    done = []
    for kept, got in pieces:
        total = (kept + after(got, total).astype(jnp.float32)).astype(jnp.float16)
        done.append(to_owner(total))
    return jnp.concatenate(done, 0).astype(jnp.float32) * (1.0 / GAIN)


def solution(mesh):
    placed = (P("pair", "ga"), P("pair"), P("pair"), P(), P())
    return jax.shard_map(
        body, mesh=mesh, in_specs=placed, out_specs=P("ga", "pair"), check_vma=False
    )
```

```python
import functools
import math

import jax
import jax.numpy as jnp
import numpy as np
from jax import lax
from jax.experimental import pallas as pl
from jax.experimental.pallas import tpu as pltpu
from jax.sharding import PartitionSpec as P


AXES = ("pair", "ga")
CUTS = (384,) * 4
GAIN = 4.0

O, N, S, Z = (0, 0), (1, 0), (3, 0), (1, 1)
EARLY = ((O, O), (O, N), (O, S), (S, N))
LATE = ((O, Z), (Z, O), (Z, N), (S, Z))
PLAN = (
    ((3, 0, 2, 1), (2, 1, 0, 3), (1, 0, 1, 0)),
    ((2, 3, 1, 0), (1, 2, 0, 3), (1, 0, 0, 1)),
    ((0, 3, 1, 2), (0, 1, 2, 3), (0, 0, 1, 0)),
    ((3, 2, 0, 1), (2, 1, 3, 0), (0, 1, 1, 1)),
    ((2, 1, 3, 0), (3, 0, 2, 1), (1, 1, 1, 0)),
    ((1, 0, 2, 3), (0, 3, 1, 2), (1, 1, 1, 0)),
    ((1, 2, 0, 3), (2, 3, 0, 1), (1, 0, 0, 0)),
    ((0, 1, 3, 2), (3, 0, 2, 1), (1, 1, 0, 1)),
)


def index(x, y, z, core):
    x, y, z = x % 4, y % 4, z % 4
    return (4 * x + 2 * (z % 2) + core) * 8 + 4 * (z // 2) + y


def devices():
    for x in range(4):
        for y in range(4):
            for z in range(4):
                for core in range(2):
                    yield x, y, z, core


def shift(value, dx=0, dy=0, dz=0, swap=False):
    pairs = [
        (index(x, y, z, c), index(x + dx, y + dy, z + dz, 1 - c if swap else c))
        for x, y, z, c in devices()
    ]
    return lax.ppermute(value, AXES, pairs)


def swap_z_lo(value):
    pairs = [(index(x, y, z, c), index(x, y, z ^ 1, c)) for x, y, z, c in devices()]
    return lax.ppermute(value, AXES, pairs)


def to_owner(value):
    pairs = []
    for x, y, z, c in devices():
        early, late, keeper = PLAN[4 * (z // 2) + y]
        keeps = keeper[x] == z % 2
        row, col = EARLY[early[x]] if keeps else LATE[late[x]]
        row_y, row_hi = (y + row[0]) % 4, (z // 2 + row[1]) % 2
        block = 4 * ((z // 2 + col[1]) % 2) + (y + col[0]) % 4
        pairs.append(
            (index(x, y, z, c), index(block // 2, row_y, 2 * row_hi + block % 2, c))
        )
    return lax.ppermute(value, AXES, pairs)


def planned(pair, ga):
    x, z_lo = pair >> 2, (pair >> 1) & 1
    word = jnp.int32(0)
    for k, (early, late, keeper) in enumerate(PLAN):
        code = sum(v << 2 * i for i, v in enumerate(early + late))
        code += sum(v << 16 + i for i, v in enumerate(keeper))
        word = jnp.where(ga == k, code, word)

    def entry(d, base):
        return (word >> (2 * ((x + d) & 3) + base)) & 3

    early, late = ([entry(d, base) for d in range(4)] for base in (0, 8))
    return early, late, ((word >> (16 + x)) & 1) == z_lo


def lookup(bands, energy):
    levels = lax.broadcasted_iota(jnp.int32, (1, energy.shape[0]), 1)
    onehot = (bands[:, None] == levels).astype(jnp.float32)
    return jnp.sum(onehot * energy[None, :], axis=1)


def placing(which):
    return [sum(jnp.where(w == s, d, 0) for d, w in enumerate(which)) for s in range(4)]


def chunk(k):
    return slice(sum(CUTS[:k]), sum(CUTS[: k + 1]))


COUNT = len(CUTS)
TAIL = (320, 512)
SPLIT = 3


def stage_kernel(late, lo, hi, n_in, *refs):
    first, last = lo == 0, hi == COUNT
    sources, refs = refs[:n_in], refs[n_in:]
    n_out = (2 if last else 1) + (not late)
    outs, (row, own_t, own, north, far, *rest, sems) = refs[:n_out], refs[n_out:]
    rows = slice(chunk(lo).start, chunk(hi - 1).stop)
    spans = [slice(chunk(k).start - rows.start, chunk(k).stop - rows.start) for k in range(lo, hi)]
    pairs = [
        (sources[0].at[:, rows], row),
        (sources[1].at[:, rows], own_t),
        (sources[2].at[rows, :], own),
        *((s, north.at[c]) for s, c in zip(sources[3:], spans)),
        *((s, far.at[c]) for s, c in zip(sources[3 + hi - lo :], spans)),
    ]
    extra = sources[len(pairs) :]
    if late:
        left, flipped = own_t, rest[0]
        size, edge = own.shape[1], chunk(SPLIT).start
        pairs[1] = (sources[1], left.at[:size])
        pairs += [
            (extra[0], left.at[size:, :edge]),
            (extra[1], left.at[size:, edge:]),
        ]
    else:
        flipped = outs[-1]
        pairs += zip(extra, rest)
    copies = [
        pltpu.make_async_copy(s, t, sems.at[i]) for i, (s, t) in enumerate(pairs)
    ]
    for copy in copies:
        copy.start()
    pair, ga = lax.axis_index("pair"), lax.axis_index("ga")
    core, at = pair & 1, placing(planned(pair, ga)[int(late)])
    half = own.shape[1] // 2

    def put(i, left, right):
        keep(i, jnp.dot(left[...], right[...], preferred_element_type=jnp.float32))

    def keep(i, total):
        if not first:
            total = total + rest[0][i]
        if last:
            low, high = total[:, :half], total[:, half:]
            outs[0][at[i]] = jnp.where(core == 0, high, low)
            outs[1][at[i]] = jnp.where(core == 0, low, high)
        else:
            outs[0][i] = total

    for copy in copies:
        copy.wait()
    if late:
        total = jnp.dot(left[...], far[...], preferred_element_type=jnp.float32)
        size = own.shape[1]
        keep(0, total[:size])
        keep(3, total[size:])
    else:
        put(0, own_t, own)
        put(1, own_t, north)
        put(2, own_t, far)
    flipped[...] = (row[...] * far[...].T.astype(jnp.float32)).astype(flipped.dtype)
    if late:
        put(1, flipped, own)
        put(2, flipped, north)
    else:
        put(3, flipped, north)


def run_stage(late, lo, hi, sources):
    size, _ = sources[1].shape
    rows = sum(CUTS[lo:hi])
    tall, wide = ((rows, size), jnp.bfloat16), ((size, rows), jnp.bfloat16)
    held = [((1, rows), jnp.float32), wide, tall, tall, tall]
    outs = [((4, size, size), jnp.float32)]
    if late:
        held[1] = ((2 * size, rows), jnp.bfloat16)
        held.append(wide)
    elif lo:
        held += outs
    if hi == COUNT:
        outs = [((4, size, size // 2), jnp.float32)] * 2
    if not late:
        outs.append(wide)
    return pl.pallas_call(
        functools.partial(stage_kernel, late, lo, hi, len(sources)),
        out_shape=[jax.ShapeDtypeStruct(*o) for o in outs],
        in_specs=[pl.BlockSpec(memory_space=pl.ANY)] * len(sources),
        out_specs=[pl.BlockSpec(memory_space=pltpu.VMEM)] * len(outs),
        scratch_shapes=[
            *(pltpu.VMEM(*h) for h in held),
            pltpu.SemaphoreType.DMA((len(sources),)),
        ],
        compiler_params=pltpu.CompilerParams(vmem_limit_bytes=28 * 2**20),
        cost_estimate=pl.CostEstimate(
            flops=8 * size * size * rows, bytes_accessed=2**23, transcendentals=0
        ),
    )(*sources)


def body(own, val_band, cond_band, val_energy, cond_energy):
    pairs_total = own.shape[0] * lax.axis_size("pair")
    pair, ga = lax.axis_index("pair"), lax.axis_index("ga")
    starts = np.cumsum((0,) + CUTS)

    def rows(block, k):
        return block[starts[k] : starts[k + 1]]

    norths, souths, farther = [], [], []
    first = rows(own, 0)
    rest = lax.optimization_barrier((own, first))[0]
    for k in range(len(CUTS)):
        piece = rows(rest, k) if k else first
        norths.append(shift(piece, dy=-1))
        souths.append(shift(piece, dy=1))
        farther.append(shift(norths[k], dz=2))

    def over_x(theirs, mine, parts):
        theirs, mine = lax.optimization_barrier(
            (theirs.astype(jnp.float16), mine.astype(jnp.float16))
        )
        theirs = shift(theirs, swap=True)
        joined = [
            mine[d].astype(jnp.float32) + theirs[d].astype(jnp.float32)
            for d in range(4)
        ]
        kept, *sent = lax.optimization_barrier(
            [joined[0]] + [joined[d].astype(jnp.float16) for d in (1, 3, 2)]
        )
        got = []
        for part in parts:
            got.append([])
            for d, value in zip((1, 3, 2), sent):
                got[-1].append(shift(value[part], dx=d))
        return kept, got

    gap = lookup(val_band, val_energy) - lookup(cond_band, cond_energy)
    weight = (4.0 * GAIN) / (gap * math.sqrt(pairs_total))
    row = weight[None, :]
    own_t = (row * own.T.astype(jnp.float32)).astype(jnp.bfloat16)
    row, own_t = lax.optimization_barrier((row, own_t))
    base = [row, own_t, own]
    tail = [slice(u, v) for u, v in zip((0, *TAIL), TAIL)]
    one, two = slice(0, SPLIT), slice(SPLIT, COUNT)

    early_sum, south_a = run_stage(False, 0, SPLIT, base + norths[one] + souths[one])
    *early, south_b = run_stage(
        False, SPLIT, COUNT, base + norths[two] + souths[two] + [early_sum]
    )
    early, early_got = over_x(*early, [slice(None)])
    late = run_stage(
        True, 0, COUNT, base + norths + farther + [south_a, south_b]
    )
    late, late_got = over_x(*late, tail)

    def sum_of(kept, got):
        return kept + sum(g.astype(jnp.float32) for g in got)

    def after(value, other):
        return value if other is None else lax.optimization_barrier((value, other))[0]

    early = lax.optimization_barrier(sum_of(early, early_got[0]))
    keeps = planned(pair, ga)[2]
    pieces, sent, total = [], None, None
    for h, part in enumerate(tail):
        whole = sum_of(late[part], after(late_got[h], sent))
        kept = jnp.where(keeps, early[part], whole)
        sent = jnp.where(keeps, whole, early[part]).astype(jnp.float16)
        pieces.append((kept, swap_z_lo(sent)))
    done = []
    for kept, got in pieces:
        total = (kept + after(got, total).astype(jnp.float32)).astype(jnp.float16)
        done.append(to_owner(total))
    return jnp.concatenate(done, 0).astype(jnp.float32) * (1.0 / GAIN)


def solution(mesh):
    placed = (P("pair", "ga"), P("pair"), P("pair"), P(), P())
    return jax.shard_map(
        body, mesh=mesh, in_specs=placed, out_specs=P("ga", "pair"), check_vma=False
    )
```

```python
import functools
import math

import jax
import jax.numpy as jnp
import numpy as np
from jax import lax
from jax.experimental import pallas as pl
from jax.experimental.pallas import tpu as pltpu
from jax.sharding import PartitionSpec as P


AXES = ("pair", "ga")
CUTS = (384,) * 4
GAIN = 4.0

O, N, S, Z = (0, 0), (1, 0), (3, 0), (1, 1)
EARLY = ((O, O), (O, N), (O, S), (S, N))
LATE = ((O, Z), (Z, O), (Z, N), (S, Z))
PLAN = (
    ((3, 0, 2, 1), (2, 1, 0, 3), (1, 0, 1, 0)),
    ((2, 3, 1, 0), (1, 2, 0, 3), (1, 0, 0, 1)),
    ((0, 3, 1, 2), (0, 1, 2, 3), (0, 0, 1, 0)),
    ((3, 2, 0, 1), (2, 1, 3, 0), (0, 1, 1, 1)),
    ((2, 1, 3, 0), (3, 0, 2, 1), (1, 1, 1, 0)),
    ((1, 0, 2, 3), (0, 3, 1, 2), (1, 1, 1, 0)),
    ((1, 2, 0, 3), (2, 3, 0, 1), (1, 0, 0, 0)),
    ((0, 1, 3, 2), (3, 0, 2, 1), (1, 1, 0, 1)),
)


def index(x, y, z, core):
    x, y, z = x % 4, y % 4, z % 4
    return (4 * x + 2 * (z % 2) + core) * 8 + 4 * (z // 2) + y


def devices():
    for x in range(4):
        for y in range(4):
            for z in range(4):
                for core in range(2):
                    yield x, y, z, core


def shift(value, dx=0, dy=0, dz=0, swap=False):
    pairs = [
        (index(x, y, z, c), index(x + dx, y + dy, z + dz, 1 - c if swap else c))
        for x, y, z, c in devices()
    ]
    return lax.ppermute(value, AXES, pairs)


def swap_z_lo(value):
    pairs = [(index(x, y, z, c), index(x, y, z ^ 1, c)) for x, y, z, c in devices()]
    return lax.ppermute(value, AXES, pairs)


def to_owner(value):
    pairs = []
    for x, y, z, c in devices():
        early, late, keeper = PLAN[4 * (z // 2) + y]
        keeps = keeper[x] == z % 2
        row, col = EARLY[early[x]] if keeps else LATE[late[x]]
        row_y, row_hi = (y + row[0]) % 4, (z // 2 + row[1]) % 2
        block = 4 * ((z // 2 + col[1]) % 2) + (y + col[0]) % 4
        pairs.append(
            (index(x, y, z, c), index(block // 2, row_y, 2 * row_hi + block % 2, c))
        )
    return lax.ppermute(value, AXES, pairs)


def planned(pair, ga):
    x, z_lo = pair >> 2, (pair >> 1) & 1
    word = jnp.int32(0)
    for k, (early, late, keeper) in enumerate(PLAN):
        code = sum(v << 2 * i for i, v in enumerate(early + late))
        code += sum(v << 16 + i for i, v in enumerate(keeper))
        word = jnp.where(ga == k, code, word)

    def entry(d, base):
        return (word >> (2 * ((x + d) & 3) + base)) & 3

    early, late = ([entry(d, base) for d in range(4)] for base in (0, 8))
    return early, late, ((word >> (16 + x)) & 1) == z_lo


def lookup(bands, energy):
    levels = lax.broadcasted_iota(jnp.int32, (1, energy.shape[0]), 1)
    onehot = (bands[:, None] == levels).astype(jnp.float32)
    return jnp.sum(onehot * energy[None, :], axis=1)


def placing(which):
    return [sum(jnp.where(w == s, d, 0) for d, w in enumerate(which)) for s in range(4)]


def chunk(k):
    return slice(sum(CUTS[:k]), sum(CUTS[: k + 1]))


COUNT = len(CUTS)
TAIL = (320, 512)
SPLIT = 3


def stage_kernel(late, lo, hi, n_in, *refs):
    first, last, n = lo == 0, hi == COUNT, hi - lo
    sources, refs = refs[:n_in], refs[n_in:]
    n_out = (2 if last else 1) + (not late)
    outs, (*flipped, north_held, far_held) = refs[:n_out], refs[n_out:]
    flipped = flipped[0] if late else outs[-1]
    rows = slice(chunk(lo).start, chunk(hi - 1).stop)
    row, own_t, own = sources[0][:, rows], sources[1], sources[2]
    extra = sources[3 + 2 * n :]

    def joined(blocks, held):
        if n == 1:
            return blocks[0]
        for k, block in zip(range(lo, hi), blocks):
            held[chunk(k).start - rows.start : chunk(k).stop - rows.start] = block[...]
        return held

    pair, ga = lax.axis_index("pair"), lax.axis_index("ga")
    core, at = pair & 1, placing(planned(pair, ga)[int(late)])
    half = own.shape[1] // 2

    def keep(i, *pairs):
        total = sum(jnp.dot(u, v, preferred_element_type=jnp.float32) for u, v in pairs)
        if not first:
            total = total + extra[0][i]
        if last:
            low, high = total[:, :half], total[:, half:]
            outs[0][at[i]] = jnp.where(core == 0, high, low)
            outs[1][at[i]] = jnp.where(core == 0, low, high)
        else:
            outs[0][i] = total

    far = joined(sources[3 + n : 3 + 2 * n], far_held)
    keep(0 if late else 2, (own_t[:, rows], far[...]))
    flipped[...] = (row * far[...].T.astype(jnp.float32)).astype(flipped.dtype)
    north = joined(sources[3 : 3 + n], north_held)
    if late:
        edge = chunk(SPLIT).start
        keep(3, (extra[0][...], far[:edge, :]), (extra[1][...], far[edge:, :]))
        keep(1, (flipped[...], own[...]))
        keep(2, (flipped[...], north[...]))
    else:
        keep(0, (own_t[:, rows], own[rows, :]))
        keep(1, (own_t[:, rows], north[...]))
        keep(3, (flipped[...], north[...]))


def run_stage(late, lo, hi, sources):
    size, _ = sources[1].shape
    rows = sum(CUTS[lo:hi])
    tall, wide = ((rows, size), jnp.bfloat16), ((size, rows), jnp.bfloat16)
    outs = [((4, size, size), jnp.float32)]
    if hi == COUNT:
        outs = [((4, size, size // 2), jnp.float32)] * 2
    if not late:
        outs.append(wide)
    return pl.pallas_call(
        functools.partial(stage_kernel, late, lo, hi, len(sources)),
        out_shape=[jax.ShapeDtypeStruct(*o) for o in outs],
        in_specs=[pl.BlockSpec(memory_space=pltpu.VMEM)] * len(sources),
        out_specs=[pl.BlockSpec(memory_space=pltpu.VMEM)] * len(outs),
        scratch_shapes=[pltpu.VMEM(*h) for h in [wide] * late + [tall, tall]],
        compiler_params=pltpu.CompilerParams(vmem_limit_bytes=40 * 2**20),
        cost_estimate=pl.CostEstimate(
            flops=8 * size * size * rows, bytes_accessed=2**23, transcendentals=0
        ),
    )(*sources)


def body(own, val_band, cond_band, val_energy, cond_energy):
    pairs_total = own.shape[0] * lax.axis_size("pair")
    pair, ga = lax.axis_index("pair"), lax.axis_index("ga")
    starts = np.cumsum((0,) + CUTS)

    def rows(block, k):
        return block[starts[k] : starts[k + 1]]

    norths, souths, farther = [], [], []
    first = rows(own, 0)
    rest = lax.optimization_barrier((own, first))[0]
    for k in range(len(CUTS)):
        piece = rows(rest, k) if k else first
        norths.append(shift(piece, dy=-1))
        souths.append(shift(piece, dy=1))
        farther.append(shift(norths[k], dz=2))

    def over_x(theirs, mine, parts):
        theirs, mine = lax.optimization_barrier(
            (theirs.astype(jnp.float16), mine.astype(jnp.float16))
        )
        theirs = shift(theirs, swap=True)
        joined = [
            mine[d].astype(jnp.float32) + theirs[d].astype(jnp.float32)
            for d in range(4)
        ]
        kept, *sent = lax.optimization_barrier(
            [joined[d].astype(jnp.float16) for d in (0, 1, 3, 2)]
        )
        got = []
        for part in parts:
            got.append([])
            for d, value in zip((1, 3, 2), sent):
                got[-1].append(shift(value[part], dx=d))
        return kept, got

    gap = lookup(val_band, val_energy) - lookup(cond_band, cond_energy)
    weight = (4.0 * GAIN) / (gap * math.sqrt(pairs_total))
    row = weight[None, :]
    own_t = (row * own.T.astype(jnp.float32)).astype(jnp.bfloat16)
    row, own_t = lax.optimization_barrier((row, own_t))
    base = [row, own_t, own]
    tail = [slice(u, v) for u, v in zip((0, *TAIL), TAIL)]
    one, two = slice(0, SPLIT), slice(SPLIT, COUNT)

    early_sum, south_a = run_stage(False, 0, SPLIT, base + norths[one] + souths[one])
    *early, south_b = run_stage(
        False, SPLIT, COUNT, base + norths[two] + souths[two] + [early_sum]
    )
    early, early_got = over_x(*early, [slice(None)])
    late = run_stage(
        True, 0, COUNT, base + norths + farther + [south_a, south_b]
    )
    late, late_got = over_x(*late, tail)

    def sum_of(kept, got):
        return kept.astype(jnp.float32) + sum(g.astype(jnp.float32) for g in got)

    def after(value, other):
        return value if other is None else lax.optimization_barrier((value, other))[0]

    early = lax.optimization_barrier(sum_of(early, early_got[0]))
    keeps = planned(pair, ga)[2]
    pieces, sent, total = [], None, None
    for h, part in enumerate(tail):
        whole = sum_of(late[part], after(late_got[h], sent))
        kept = jnp.where(keeps, early[part], whole)
        sent = jnp.where(keeps, whole, early[part]).astype(jnp.float16)
        pieces.append((kept, swap_z_lo(sent)))
    done = []
    for kept, got in pieces:
        total = (kept + after(got, total).astype(jnp.float32)).astype(jnp.float16)
        done.append(to_owner(total))
    return jnp.concatenate(done, 0).astype(jnp.float32) * (1.0 / GAIN)


def solution(mesh):
    placed = (P("pair", "ga"), P("pair"), P("pair"), P(), P())
    return jax.shard_map(
        body, mesh=mesh, in_specs=placed, out_specs=P("ga", "pair"), check_vma=False
    )
```
